32 devices in a mesh: blk: 8 (over y, x, core), layer: 4 (over z).
Axes of the slice: x: 2, y: 2, z: 4, core: 2. Of those that a mesh axis runs over, the one named last changes fastest.
Arguments:
- points: float32 [8192, 128], P('blk'), may hold values from -6 to 6
- inv_scale: float32 [128], replicated, may hold values from 0.01 to 0.25
- vectors: float32 [8192, 64], P('blk'), may hold values from -6 to 6
- noise: float32 [8192], P(('blk', 'layer')), may hold values from 0.1 to 1
Outputs:
- result: float32 [8192, 64], P(('blk', 'layer'))
The draws below stay inside these ranges and needn't reach their ends.
All inputs are finite; a program needn't handle non-finite values.
Results may differ from the reference program's by a relative error of at most 0.0001.
Values sent between devices are 32-bit elements; how exact they have to be, the bound alone decides.
A program may use at most 64 MiB of HBM per device.

```python
import math
import jax
import jax.numpy as jnp
from jax import lax

FEATS = 128
RHS = 64
BLOCK = 1024
NPTS = 8192
N_BLK = 8
N_LAYER = 4


def shard_levels(stream_key, dims, pieces, low, top_value):
    gain, own = 1.0, jax.random.fold_in(stream_key, 6)
    for axis_at, blocks in pieces:
        draws = jnp.exp(jax.random.uniform(jax.random.fold_in(own, axis_at), (blocks,), jnp.float32, low / len(pieces), top_value / len(pieces)))
        gain = gain * jnp.repeat(draws, dims[axis_at] // blocks).reshape([-1 if axis == axis_at else 1 for axis in range(len(dims))])
    return gain


def centred(own_key, extent, deviation, reach, pieces=(), held_as=jnp.bfloat16):
    gain = shard_levels(own_key, extent, pieces, -0.22, 0.18) if pieces else 1.0
    result = jax.random.normal(own_key, extent, jnp.float32) * deviation * gain
    return jnp.minimum(jnp.maximum(result, -reach), reach).astype(held_as)


def setup_inputs(seed: int = 0) -> dict:
    key_of = jax.random.split(jax.random.key(seed), 5)
    return {
        "points": centred(key_of[0], (NPTS, FEATS), 1.0, 6.0, ((0, 8),), jnp.float32),
        "inv_scale": jnp.clip(jnp.exp(jax.random.uniform(key_of[1], (FEATS,), jnp.float32, math.log(0.01), math.log(0.25))), 0.01, 0.25),
        "vectors": centred(key_of[2], (NPTS, RHS), 1.0, 6.0, ((0, 8),), jnp.float32),
        "noise": jnp.clip(jnp.exp(math.log(1.0) - 2.3025851 * jax.random.uniform(key_of[3], (NPTS,), jnp.float32) ** shard_levels(key_of[3], (NPTS,), ((0, 32),), -0.2, 0.2)), 0.1, 1.0),
    }


ROOT_FIVE = 5.0 ** 0.5
FIVE_THIRDS = 5.0 / 3.0

def matern(left_scaled, right_scaled):
    left_norms = lax.optimization_barrier(jnp.sum(left_scaled * left_scaled, axis=1))
    right_norms = lax.optimization_barrier(jnp.sum(right_scaled * right_scaled, axis=1))
    cross = jnp.dot(left_scaled, right_scaled.T, precision=lax.Precision.HIGHEST, preferred_element_type=jnp.float32)
    distance_sq = jnp.maximum(left_norms[:, None] + right_norms[None, :] - 2.0 * cross, 0.0)
    radius = jnp.sqrt(distance_sq)
    return (1.0 + ROOT_FIVE * radius + FIVE_THIRDS * distance_sq) * jnp.exp(-ROOT_FIVE * radius)

def tile_pair(members):
    left_scaled, right_scaled, left_vectors, right_vectors = members
    kernel = matern(left_scaled, right_scaled)
    direct = jnp.dot(kernel, right_vectors, precision=lax.Precision.HIGHEST, preferred_element_type=jnp.float32)
    mirrored = jnp.dot(kernel.T, left_vectors, precision=lax.Precision.HIGHEST, preferred_element_type=jnp.float32)
    return (direct, mirrored)

def reference(points, inv_scale, vectors, noise):
    scaled = (points * inv_scale[None, :]).reshape(N_BLK, BLOCK, FEATS)
    grouped = vectors.reshape(N_BLK, BLOCK, RHS)
    summed = jnp.zeros((N_BLK, BLOCK, RHS), jnp.float32)
    for distance in range(N_LAYER):
        partner_scaled = jnp.roll(scaled, -distance, axis=0)
        partner_vectors = jnp.roll(grouped, -distance, axis=0)
        direct, mirrored = lax.map(tile_pair, (scaled, partner_scaled, grouped, partner_vectors))
        summed = summed + direct
        if distance > 0:
            summed = summed + jnp.roll(mirrored, distance, axis=0)
    normalizer = float(BLOCK * (2 * N_LAYER - 1)) ** (-0.5)
    return summed.reshape(NPTS, RHS) * normalizer + noise[:, None] * vectors
```

```python
import functools
import math

import jax
import jax.numpy as jnp
from jax import lax
from jax.experimental import pallas as pl
from jax.experimental.pallas import tpu as pltpu
from jax.sharding import PartitionSpec as P

MESH = pl.DeviceIdType.MESH
LOG2 = math.log(2.0)
UNIT = math.sqrt(5.0) / LOG2
BF16 = jnp.bfloat16
F32 = jnp.float32


def two_terms(value):
    high = value.astype(BF16).astype(F32)
    return high, (value - high).astype(BF16).astype(F32)


def augmented(points, scale, left):
    high, low = two_terms(points * scale)
    held = high + low
    norm = jnp.sum(held * held, axis=1, keepdims=True)
    first = norm.astype(BF16).astype(F32)
    second = (norm - first).astype(BF16).astype(F32)
    third = norm - first - second
    lane = lax.broadcasted_iota(jnp.int32, high.shape, 1)
    at, ones = (0, 3) if left else (3, 0)
    extra = jnp.where(
        lane == at,
        first,
        jnp.where(
            lane == at + 1,
            second,
            jnp.where(
                lane == at + 2,
                third,
                jnp.where((lane >= ones) & (lane < ones + 3), 1.0, 0.0),
            ),
        ),
    )
    if left:
        high, low = -2.0 * high, -2.0 * low
        terms = (high, high, low, extra)
    else:
        terms = (high, low, high, extra)
    return jnp.concatenate([term.astype(BF16) for term in terms], axis=1)


def nt_dot(left, right):
    return lax.dot_general(left, right, (((1,), (1,)), ((), ())), preferred_element_type=F32)


def kernel(
    blocks, layers, tile, points, scale, vectors, noise, out,
    p_own, v_own, p_in, v_in, left, v_left, direct, m_out, d_out, m_in, d_in,
    own_sem, p_send, v_send, p_recv, v_recv, pf_send, vf_send, m_send, m_recv, d_send, d_recv,
):
    block, layer = lax.axis_index("blk"), lax.axis_index("layer")
    core = lax.rem(block, 2)
    sibling = block + 1 - 2 * core
    rows, columns = p_own.shape[0], v_own.shape[0]
    piece = rows // layers

    def wrapped(index):
        return lax.rem(index + 2 * blocks, blocks)

    first_core = block - core
    partner = jnp.where(
        layer == 0,
        block,
        jnp.where(
            layer == 1,
            jnp.where(core == 0, block + 1, wrapped(block + layers - 1)),
            wrapped(first_core + layer),
        ),
    )
    shares = layer >= 2
    spreads = shares & (core == lax.rem(layer, 2))
    sends = (layer == 1) | spreads

    own_p = pltpu.make_async_copy(points, p_own, own_sem.at[0])
    own_v = pltpu.make_async_copy(vectors, v_own, own_sem.at[1])
    own_p.start()
    own_v.start()

    @pl.when(layer == 0)
    def _():
        for c in range(layers):
            at = pl.ds(c * piece, piece)
            pltpu.make_async_copy(points.at[at], p_in.at[c], p_recv.at[c]).start()
            pltpu.make_async_copy(vectors.at[:, at], v_in.at[c], v_recv.at[c]).start()

    barrier = pltpu.get_barrier_semaphore()

    def greet(to_block, to_layer):
        pl.semaphore_signal(barrier, inc=1, device_id=(to_block, to_layer), device_id_type=MESH)

    @pl.when(layer == 1)
    def _():
        greet(partner, layer)

    @pl.when(shares)
    def _():
        greet(partner, layer)
        greet(sibling, layer)

    for other in range(layers):

        @pl.when(layer != other)
        def _():
            greet(block, other)

    greet(wrapped(jnp.where(core == 1, block - 1, block - (layers - 1))), 1)
    for other in range(2, layers):

        @pl.when(core == other % 2)
        def _():
            greet(wrapped(block - other), other)
            greet(wrapped(block - other + 1), other)

    expected = layers - 1
    expected += jnp.where(layer >= 1, layers, 0) + jnp.where(sends, 1, 0)
    expected += jnp.where(shares, 1, 0) + jnp.where(spreads, 1, 0)
    pl.semaphore_wait(barrier, expected)

    own_p.wait()
    own_v.wait()

    def far(c):
        at = pl.ds(c * piece, piece)
        target = wrapped(
            jnp.where(
                layer == 1,
                jnp.where(core == 1, block - 1, block - (layers - 1)),
                block - layer + c % 2,
            )
        )
        return (
            pltpu.make_async_remote_copy(
                p_own.at[at], p_in.at[c], p_send.at[c], p_recv.at[c], (target, layer), MESH
            ),
            pltpu.make_async_remote_copy(
                v_own.at[:, at], v_in.at[c], v_send.at[c], v_recv.at[c], (target, layer), MESH
            ),
        )

    def near(c):
        return (
            pltpu.make_async_remote_copy(
                p_in.at[c], p_in.at[c], pf_send.at[c], p_recv.at[c], (sibling, layer), MESH
            ),
            pltpu.make_async_remote_copy(
                v_in.at[c], v_in.at[c], vf_send.at[c], v_recv.at[c], (sibling, layer), MESH
            ),
        )

    slot = jnp.where(layer == 1, 0, 1 + 2 * (layer // 2 - 1) + core)

    def mirrored_copy(c):
        return pltpu.make_async_remote_copy(
            m_out.at[c], m_in.at[slot], m_send.at[c], m_recv.at[slot], (partner, c), MESH
        )

    def direct_copy(c):
        return pltpu.make_async_remote_copy(
            d_out.at[c], d_in.at[layer], d_send.at[c], d_recv.at[layer], (block, c), MESH
        )

    @pl.when(sends)
    def _():
        for c in range(layers):
            for copy in far(c):
                copy.start()

    unit = scale[...] * UNIT
    left[...] = augmented(p_own[...], unit, True)
    v_left[...] = jnp.concatenate(two_terms(v_own[...]), axis=0).astype(BF16)

    for c in range(layers):
        pltpu.make_async_copy(p_in.at[c], p_in.at[c], p_recv.at[c]).wait()
        pltpu.make_async_copy(v_in.at[c], v_in.at[c], v_recv.at[c]).wait()

        @pl.when(shares & (core == c % 2))
        def _():
            for copy in near(c):
                copy.start()

        right = augmented(p_in[c], unit, False)
        v_right = jnp.concatenate(two_terms(v_in[c]), axis=0).T.astype(BF16)
        mirrored = None
        for start in range(0, rows, tile):
            at = pl.ds(start, tile)
            square = jnp.maximum(nt_dot(left[at, :], right), 1e-20)
            u = square * lax.rsqrt(square)
            value = (1.0 + u * (LOG2 + u * (LOG2 * LOG2 / 3.0))) * jnp.exp2(-u)
            high = value.astype(BF16)
            low = (value - high.astype(F32)).astype(BF16)
            term = jnp.dot(high, v_right, preferred_element_type=F32)
            term += jnp.dot(low, v_right, preferred_element_type=F32)
            if c == 0:
                direct[at, :] = term
            else:
                direct[at, :] += term
            turned = jnp.dot(v_left[:, at], high, preferred_element_type=F32)
            turned += jnp.dot(v_left[:, at], low, preferred_element_type=F32)
            mirrored = turned if mirrored is None else mirrored + turned
        m_out[c] = mirrored[:columns] + mirrored[columns:]

        @pl.when(layer >= 1)
        def _():
            mirrored_copy(c).start()

    for c in range(layers):
        turned = direct[pl.ds(c * piece, piece), :].T
        turned = turned[:columns] + turned[columns:]

        @pl.when(layer == c)
        def _():
            d_in[c] = turned

        @pl.when(layer != c)
        def _():
            d_out[c] = turned
            direct_copy(c).start()

    for s in range(layers - 1):
        pltpu.make_async_copy(m_in.at[s], m_in.at[s], m_recv.at[s]).wait()
    total = m_in[0]
    for s in range(1, layers - 1):
        total += m_in[s]
    for s in range(layers):

        @pl.when(layer != s)
        def _():
            pltpu.make_async_copy(d_in.at[s], d_in.at[s], d_recv.at[s]).wait()

    for s in range(layers):
        total += d_in[s]
    mine = v_own[:, pl.ds(pl.multiple_of(layer * piece, 128), piece)]
    normalizer = float(rows * (2 * layers - 1)) ** (-0.5)
    out[...] = total * normalizer + noise[...] * mine

    @pl.when(sends)
    def _():
        for c in range(layers):
            for copy in far(c):
                copy.wait_send()

    for c in range(layers):

        @pl.when(shares & (core == c % 2))
        def _():
            for copy in near(c):
                copy.wait_send()

        @pl.when(layer >= 1)
        def _():
            mirrored_copy(c).wait_send()

        @pl.when(layer != c)
        def _():
            direct_copy(c).wait_send()


def per_device(points, inv_scale, vectors, noise):
    blocks, layers = lax.axis_size("blk"), lax.axis_size("layer")
    rows, features = points.shape
    columns = vectors.shape[1]
    piece = rows // layers
    tile = min(256, rows)
    vmem = pl.BlockSpec(memory_space=pltpu.VMEM)
    hbm = pl.BlockSpec(memory_space=pl.ANY)
    dma = pltpu.SemaphoreType.DMA
    out = pl.pallas_call(
        functools.partial(kernel, blocks, layers, tile),
        out_shape=jax.ShapeDtypeStruct((columns, piece), F32),
        in_specs=[hbm, vmem, hbm, vmem],
        out_specs=vmem,
        scratch_shapes=[
            pltpu.VMEM((rows, features), F32),
            pltpu.VMEM((columns, rows), F32),
            pltpu.VMEM((layers, piece, features), F32),
            pltpu.VMEM((layers, columns, piece), F32),
            pltpu.VMEM((rows, 4 * features), BF16),
            pltpu.VMEM((2 * columns, rows), BF16),
            pltpu.VMEM((rows, 2 * columns), F32),
            pltpu.VMEM((layers, columns, piece), F32),
            pltpu.VMEM((layers, columns, piece), F32),
            pltpu.VMEM((layers - 1, columns, piece), F32),
            pltpu.VMEM((layers, columns, piece), F32),
            dma((2,)),
            *[dma((layers,)) for _ in range(7)],
            dma((layers - 1,)),
            dma((layers,)),
            dma((layers,)),
        ],
        compiler_params=pltpu.CompilerParams(collective_id=0, has_side_effects=True),
    )(points, inv_scale[None, :], vectors.T, noise[None, :])
    return out.T


def solution(mesh):
    placed = (P("blk", None), P(), P("blk", None), P(("blk", "layer")))
    return jax.shard_map(
        per_device, mesh=mesh, in_specs=placed, out_specs=P(("blk", "layer"), None), check_vma=False
    )
```

```python
import functools
import math

import jax
import jax.numpy as jnp
from jax import lax
from jax.experimental import pallas as pl
from jax.experimental.pallas import tpu as pltpu
from jax.sharding import PartitionSpec as P

MESH = pl.DeviceIdType.MESH
LOG2 = math.log(2.0)
UNIT = math.sqrt(5.0) / LOG2
BF16 = jnp.bfloat16
F32 = jnp.float32


def two_terms(value):
    high = value.astype(BF16).astype(F32)
    return high, (value - high).astype(BF16).astype(F32)


def augmented(points, scale, left):
    high, low = two_terms(points * scale)
    held = high + low
    norm = jnp.sum(held * held, axis=1, keepdims=True)
    first = norm.astype(BF16).astype(F32)
    second = (norm - first).astype(BF16).astype(F32)
    third = norm - first - second
    lane = lax.broadcasted_iota(jnp.int32, high.shape, 1)
    at, ones = (0, 3) if left else (3, 0)
    extra = jnp.where(
        lane == at,
        first,
        jnp.where(
            lane == at + 1,
            second,
            jnp.where(
                lane == at + 2,
                third,
                jnp.where((lane >= ones) & (lane < ones + 3), 1.0, 0.0),
            ),
        ),
    )
    if left:
        high, low = -2.0 * high, -2.0 * low
        terms = (high, high, low, extra)
    else:
        terms = (high, low, high, extra)
    return jnp.concatenate([term.astype(BF16) for term in terms], axis=1)


def nt_dot(left, right):
    return lax.dot_general(left, right, (((1,), (1,)), ((), ())), preferred_element_type=F32)


def kernel(
    blocks, layers, tile, points, scale, vectors, noise, out,
    p_own, v_own, p_in, v_in, left, v_left, direct, m_out, d_out, m_in, d_in, m_near, m_sum,
    own_sem, p_send, v_send, p_recv, v_recv, pf_send, vf_send, m_send, m_recv, d_send, d_recv, mn_send, mn_recv,
):
    block, layer = lax.axis_index("blk"), lax.axis_index("layer")
    core = lax.rem(block, 2)
    sibling = block + 1 - 2 * core
    rows, columns = p_own.shape[0], v_own.shape[0]
    piece = rows // layers

    def wrapped(index):
        return lax.rem(index + 2 * blocks, blocks)

    first_core = block - core
    partner = jnp.where(
        layer == 0,
        block,
        jnp.where(
            layer == 1,
            jnp.where(core == 0, block + 1, wrapped(block + layers - 1)),
            wrapped(first_core + layer),
        ),
    )
    shares = layer >= 2
    spreads = shares & (core == lax.rem(layer, 2))
    sends = (layer == 1) | spreads

    own_p = pltpu.make_async_copy(points, p_own, own_sem.at[0])
    own_v = pltpu.make_async_copy(vectors, v_own, own_sem.at[1])
    own_p.start()
    own_v.start()

    @pl.when(layer == 0)
    def _():
        for c in range(layers):
            at = pl.ds(c * piece, piece)
            pltpu.make_async_copy(points.at[at], p_in.at[c], p_recv.at[c]).start()
            pltpu.make_async_copy(vectors.at[:, at], v_in.at[c], v_recv.at[c]).start()

    barrier = pltpu.get_barrier_semaphore()

    def greet(to_block, to_layer):
        pl.semaphore_signal(barrier, inc=1, device_id=(to_block, to_layer), device_id_type=MESH)

    @pl.when(layer == 1)
    def _():
        greet(partner, layer)

    @pl.when(shares)
    def _():
        greet(partner, layer)
        greet(sibling, layer)

    for other in range(layers):

        @pl.when(layer != other)
        def _():
            greet(block, other)

    greet(wrapped(jnp.where(core == 1, block - 1, block - (layers - 1))), 1)
    for other in range(2, layers):

        @pl.when(core == other % 2)
        def _():
            greet(wrapped(block - other + lax.rem(layer, 2)), other)

    expected = layers - 1
    expected += jnp.where(shares, layers // 2, jnp.where(layer == 1, layers, 0)) + jnp.where(sends, 1, 0)
    expected += jnp.where(shares, 1, 0) + jnp.where(spreads, 1, 0)
    pl.semaphore_wait(barrier, expected)

    own_p.wait()
    own_v.wait()

    def far(c):
        at = pl.ds(c * piece, piece)
        target = wrapped(
            jnp.where(
                layer == 1,
                jnp.where(core == 1, block - 1, block - (layers - 1)),
                block - layer + c % 2,
            )
        )
        return (
            pltpu.make_async_remote_copy(
                p_own.at[at], p_in.at[c], p_send.at[c], p_recv.at[c], (target, layer), MESH
            ),
            pltpu.make_async_remote_copy(
                v_own.at[:, at], v_in.at[c], v_send.at[c], v_recv.at[c], (target, layer), MESH
            ),
        )

    def near(c):
        return (
            pltpu.make_async_remote_copy(
                p_in.at[c], p_in.at[c], pf_send.at[c], p_recv.at[c], (sibling, layer), MESH
            ),
            pltpu.make_async_remote_copy(
                v_in.at[c], v_in.at[c], vf_send.at[c], v_recv.at[c], (sibling, layer), MESH
            ),
        )

    slot = layer // 2

    def mirrored_copy(c):
        return pltpu.make_async_remote_copy(
            m_sum.at[c], m_in.at[slot], m_send.at[c], m_recv.at[slot], (partner, c), MESH
        )

    def mirrored_near(c):
        return pltpu.make_async_remote_copy(
            m_out.at[c], m_near.at[c], mn_send.at[c], mn_recv.at[c], (sibling, layer), MESH
        )

    def join(c):
        @pl.when(shares & (core == c % 2))
        def _():
            pltpu.make_async_copy(m_near.at[c], m_near.at[c], mn_recv.at[c]).wait()
            m_sum[c] = m_sum[c] + m_near[c]
            mirrored_copy(c).start()

    def direct_copy(c):
        return pltpu.make_async_remote_copy(
            d_out.at[c], d_in.at[layer], d_send.at[c], d_recv.at[layer], (block, c), MESH
        )

    @pl.when(sends)
    def _():
        for c in range(layers):
            for copy in far(c):
                copy.start()

    unit = scale[...] * UNIT
    left[...] = augmented(p_own[...], unit, True)
    v_left[...] = jnp.concatenate(two_terms(v_own[...]), axis=0).astype(BF16)

    for c in range(layers):
        pltpu.make_async_copy(p_in.at[c], p_in.at[c], p_recv.at[c]).wait()
        pltpu.make_async_copy(v_in.at[c], v_in.at[c], v_recv.at[c]).wait()

        @pl.when(shares & (core == c % 2))
        def _():
            for copy in near(c):
                copy.start()

        right = augmented(p_in[c], unit, False)
        v_right = jnp.concatenate(two_terms(v_in[c]), axis=0).T.astype(BF16)
        mirrored = None
        for start in range(0, rows, tile):
            at = pl.ds(start, tile)
            square = jnp.maximum(nt_dot(left[at, :], right), 1e-20)
            u = square * lax.rsqrt(square)
            value = (1.0 + u * (LOG2 + u * (LOG2 * LOG2 / 3.0))) * jnp.exp2(-u)
            high = value.astype(BF16)
            low = (value - high.astype(F32)).astype(BF16)
            term = jnp.dot(high, v_right, preferred_element_type=F32)
            term += jnp.dot(low, v_right, preferred_element_type=F32)
            if c == 0:
                direct[at, :] = term
            else:
                direct[at, :] += term
            turned = jnp.dot(v_left[:, at], high, preferred_element_type=F32)
            turned += jnp.dot(v_left[:, at], low, preferred_element_type=F32)
            mirrored = turned if mirrored is None else mirrored + turned
        mirrored = mirrored[:columns] + mirrored[columns:]

        @pl.when(shares & (core != c % 2))
        def _():
            m_out[c] = mirrored
            mirrored_near(c).start()

        @pl.when(jnp.logical_not(shares & (core != c % 2)))
        def _():
            m_sum[c] = mirrored

        @pl.when(layer == 1)
        def _():
            mirrored_copy(c).start()

        if c > 0:
            join(c - 1)

    for c in range(layers):
        turned = direct[pl.ds(c * piece, piece), :].T
        turned = turned[:columns] + turned[columns:]

        @pl.when(layer == c)
        def _():
            d_in[c] = turned

        @pl.when(layer != c)
        def _():
            d_out[c] = turned
            direct_copy(c).start()

    join(layers - 1)
    for s in range(layers // 2):
        pltpu.make_async_copy(m_in.at[s], m_in.at[s], m_recv.at[s]).wait()
    total = m_in[0]
    for s in range(1, layers // 2):
        total += m_in[s]
    for s in range(layers):

        @pl.when(layer != s)
        def _():
            pltpu.make_async_copy(d_in.at[s], d_in.at[s], d_recv.at[s]).wait()

    for s in range(layers):
        total += d_in[s]
    mine = v_own[:, pl.ds(pl.multiple_of(layer * piece, 128), piece)]
    normalizer = float(rows * (2 * layers - 1)) ** (-0.5)
    out[...] = total * normalizer + noise[...] * mine

    @pl.when(sends)
    def _():
        for c in range(layers):
            for copy in far(c):
                copy.wait_send()

    for c in range(layers):

        @pl.when(shares & (core == c % 2))
        def _():
            for copy in near(c):
                copy.wait_send()

        @pl.when((layer == 1) | (shares & (core == c % 2)))
        def _():
            mirrored_copy(c).wait_send()

        @pl.when(shares & (core != c % 2))
        def _():
            mirrored_near(c).wait_send()

        @pl.when(layer != c)
        def _():
            direct_copy(c).wait_send()


def per_device(points, inv_scale, vectors, noise):
    blocks, layers = lax.axis_size("blk"), lax.axis_size("layer")
    rows, features = points.shape
    columns = vectors.shape[1]
    piece = rows // layers
    tile = min(256, rows)
    vmem = pl.BlockSpec(memory_space=pltpu.VMEM)
    hbm = pl.BlockSpec(memory_space=pl.ANY)
    dma = pltpu.SemaphoreType.DMA
    out = pl.pallas_call(
        functools.partial(kernel, blocks, layers, tile),
        out_shape=jax.ShapeDtypeStruct((columns, piece), F32),
        in_specs=[hbm, vmem, hbm, vmem],
        out_specs=vmem,
        scratch_shapes=[
            pltpu.VMEM((rows, features), F32),
            pltpu.VMEM((columns, rows), F32),
            pltpu.VMEM((layers, piece, features), F32),
            pltpu.VMEM((layers, columns, piece), F32),
            pltpu.VMEM((rows, 4 * features), BF16),
            pltpu.VMEM((2 * columns, rows), BF16),
            pltpu.VMEM((rows, 2 * columns), F32),
            pltpu.VMEM((layers, columns, piece), F32),
            pltpu.VMEM((layers, columns, piece), F32),
            pltpu.VMEM((layers // 2, columns, piece), F32),
            pltpu.VMEM((layers, columns, piece), F32),
            pltpu.VMEM((layers, columns, piece), F32),
            pltpu.VMEM((layers, columns, piece), F32),
            dma((2,)),
            *[dma((layers,)) for _ in range(7)],
            dma((layers // 2,)),
            *[dma((layers,)) for _ in range(4)],
        ],
        compiler_params=pltpu.CompilerParams(collective_id=0, has_side_effects=True),
    )(points, inv_scale[None, :], vectors.T, noise[None, :])
    return out.T


def solution(mesh):
    placed = (P("blk", None), P(), P("blk", None), P(("blk", "layer")))
    return jax.shard_map(
        per_device, mesh=mesh, in_specs=placed, out_specs=P(("blk", "layer"), None), check_vma=False
    )
```
